512 devices in a mesh: cell: 64 (over x, z), sens: 8 (over y, core).
Axes of the slice: x: 4, y: 4, z: 16, core: 2. Of those that a mesh axis runs over, the one named last changes fastest.
Arguments:
- replicas: bfloat16 [64, 2, 64, 131072], P(None, None, 'sens', 'cell'), may hold values from -6 to 6
- csm: float32 [64, 2, 64, 64], P('cell'), as said below
Outputs:
- power: float32 [131072], P(('cell', 'sens'))
The draws below stay inside these ranges and needn't reach their ends.
Inputs may be any that keep to these rules, and one draw needn't show every extreme that they name: For each frequency the matrix csm[f, 0] + i csm[f, 1] is Hermitian and positive definite.
All inputs are finite; a program needn't handle non-finite values.
Results may differ from the reference program's by a relative error of at most 0.00035.
Values may be sent and summed in bfloat16 or wider, within the bound.
A program may use at most 64 MiB of HBM per device.

```python
import math
import jax
import jax.numpy as jnp
from jax import lax

S = 64
F = 64
CELLS = 131072


def drawn(key):
    key_cells = jax.random.fold_in(key, 21)
    key_waves = jax.random.fold_in(key, 22)
    spacing = CELLS // 3
    offsets = jax.random.randint(key_cells, (3,), 0, spacing)
    source_cells = offsets + spacing * jnp.arange(3, dtype=jnp.int32)
    source_waves = jnp.clip(jax.random.normal(key_waves, (F, 2, S, 3), jnp.float32), -6.0, 6.0)
    return (source_cells, source_waves)


def draw_replicas(key, part):
    source_cells, source_waves = drawn(key)
    fields = jax.random.normal(jax.random.fold_in(key, 1), (F, 2, S, CELLS), jnp.float32)
    fields = jnp.clip(fields, -6.0, 6.0)
    fields = fields.at[:, :, :, source_cells].set(source_waves)
    return fields.astype(jnp.bfloat16)


def draw_csm(key, part):
    snapshots = 4 * S
    source_waves = drawn(key)[1]
    key_real = jax.random.fold_in(key, 11)
    key_imag = jax.random.fold_in(key, 12)
    key_scale = jax.random.fold_in(key, 13)
    key_strength = jax.random.fold_in(key, 15)
    key_breal = jax.random.fold_in(key, 16)
    key_bimag = jax.random.fold_in(key, 17)
    real_n = jax.random.normal(key_real, (F, S, snapshots), jnp.float32)
    imag_n = jax.random.normal(key_imag, (F, S, snapshots), jnp.float32)
    strength = jnp.exp(jax.random.uniform(key_strength, (F, 1, 3), jnp.float32, math.log(1.2), math.log(3.0)))
    amplitude = jnp.sqrt(strength / (2.0 * S))
    real_a = source_waves[:, 0] * amplitude
    imag_a = source_waves[:, 1] * amplitude
    real_b = jax.random.normal(key_breal, (F, 3, snapshots), jnp.float32)
    imag_b = jax.random.normal(key_bimag, (F, 3, snapshots), jnp.float32)
    real_x = real_n + jnp.einsum('fsk,fkm->fsm', real_a, real_b) - jnp.einsum('fsk,fkm->fsm', imag_a, imag_b)
    imag_x = imag_n + jnp.einsum('fsk,fkm->fsm', real_a, imag_b) + jnp.einsum('fsk,fkm->fsm', imag_a, real_b)
    real_k = (jnp.einsum('fsm,ftm->fst', real_x, real_x) + jnp.einsum('fsm,ftm->fst', imag_x, imag_x)) / snapshots
    imag_k = (jnp.einsum('fsm,ftm->fst', imag_x, real_x) - jnp.einsum('fsm,ftm->fst', real_x, imag_x)) / snapshots
    real_k = real_k + 0.1 * jnp.eye(S, dtype=jnp.float32)[None]
    scales = jnp.exp(jax.random.uniform(key_scale, (F, 1, 1), jnp.float32, 0.0, 2.3))
    return jnp.stack([real_k * scales, imag_k * scales], axis=1)


def setup_inputs(seed: int = 0) -> dict:
    arg_keys = jax.random.split(jax.random.key(seed), 3)
    replicas = draw_replicas(jax.random.fold_in(arg_keys[2], 71), 0)
    csm = draw_csm(jax.random.fold_in(arg_keys[2], 71), 0)
    return {"replicas": replicas, "csm": csm}


def reference(replicas, csm):
    trace = jnp.sum(jnp.diagonal(csm[:, 0], axis1=1, axis2=2), axis=1)
    scaled = (csm / trace[:, None, None, None]).astype(jnp.bfloat16)

    def single(pair):
        matrix, waves = pair
        real_k, imag_k = matrix[0], matrix[1]
        real_w, imag_w = waves[0], waves[1]
        real_y = jnp.dot(real_k, real_w, preferred_element_type=jnp.float32) - jnp.dot(imag_k, imag_w, preferred_element_type=jnp.float32)
        imag_y = jnp.dot(real_k, imag_w, preferred_element_type=jnp.float32) + jnp.dot(imag_k, real_w, preferred_element_type=jnp.float32)
        real_f = real_w.astype(jnp.float32)
        imag_f = imag_w.astype(jnp.float32)
        numer = jnp.sum(real_f * real_y + imag_f * imag_y, axis=0)
        denom = jnp.sum(real_f * real_f + imag_f * imag_f, axis=0)
        return numer / denom

    terms = lax.map(single, (scaled, replicas))
    total = jnp.sum(terms, axis=0)
    return total / jnp.max(total)
```

```python
import functools

import jax
import jax.numpy as jnp
from jax import lax
from jax.experimental import pallas as pl
from jax.experimental.pallas import tpu as pltpu
from jax.sharding import Mesh
from jax.sharding import PartitionSpec as P

MESH = pl.DeviceIdType.MESH
CELL = ("cx", "cz")
SENS = ("sy", "sc")
ALL = ("cx", "cz", "sy", "sc")

CHUNKS = 8


def kernel(
    sizes,
    waves_hbm,
    csm_hbm,
    out_ref,
    csm_vmem,
    waves,
    mats,
    peak_s,
    peak_z,
    peak_x,
    local_sem,
    wave_send,
    wave_recv,
    z_send,
    z_recv,
    x_send,
    x_recv,
    ps_send,
    ps_recv,
    pz_send,
    pz_recv,
    px_send,
    px_recv,
):
    nx, nz, ny, nc = sizes
    ns = ny * nc
    cx, cz = lax.axis_index("cx"), lax.axis_index("cz")
    sy, sc = lax.axis_index("sy"), lax.axis_index("sc")
    me = sy * nc + sc
    freqs, _, rows, _ = waves_hbm.shape
    cells = waves.shape[-1]
    step = freqs // CHUNKS

    def at_s(s):
        return {"cx": cx, "cz": cz, "sy": s // nc, "sc": s % nc}

    def at_z(z):
        return {"cx": cx, "cz": z, "sy": sy, "sc": sc}

    def at_x(x):
        return {"cx": x, "cz": cz, "sy": sy, "sc": sc}

    sens_peers = [lax.rem(me + i, ns) for i in range(1, ns)]
    z_peers = [lax.rem(cz + i, nz) for i in range(1, nz)]
    x_peers = [lax.rem(cx + i, nx) for i in range(1, nx)]

    csm_in = pltpu.make_async_copy(csm_hbm.at[0], csm_vmem, local_sem.at[0])
    csm_in.start()

    def own_block(s):
        return pl.ds(pl.multiple_of(s * cells, cells), cells)

    keep = pltpu.make_async_copy(waves_hbm.at[:, :, :, own_block(me)], waves.at[me], local_sem.at[1])
    keep.start()

    barrier = pltpu.get_barrier_semaphore()
    for s in sens_peers:
        pl.semaphore_signal(barrier, inc=1, device_id=at_s(s), device_id_type=MESH)
    for x in x_peers:
        pl.semaphore_signal(barrier, inc=1, device_id=at_x(x), device_id_type=MESH)
    for z in z_peers:
        pl.semaphore_signal(barrier, inc=1, device_id=at_z(z), device_id_type=MESH)

    csm_in.wait()
    real, imag = csm_vmem[0], csm_vmem[1]
    side = real.shape[0]
    diag = lax.broadcasted_iota(jnp.int32, (side, side), 0) == lax.broadcasted_iota(jnp.int32, (side, side), 1)
    trace = jnp.sum(jnp.where(diag, real, 0.0))
    mats[cx, cz] = jnp.concatenate([real / trace, imag / trace], axis=1).astype(jnp.bfloat16)

    pl.semaphore_wait(barrier, len(sens_peers) + len(x_peers) + len(z_peers))

    def wave_copy(chunk, i, to, frm):
        part = pl.ds(chunk * step, step)
        return pltpu.make_async_remote_copy(
            src_ref=waves_hbm.at[part, :, :, own_block(to)],
            dst_ref=waves.at[frm, part],
            send_sem=wave_send.at[chunk, i],
            recv_sem=wave_recv.at[chunk, i],
            device_id=at_s(to),
            device_id_type=MESH,
        )

    for chunk in range(CHUNKS):
        for i, s in enumerate(sens_peers):
            wave_copy(chunk, i, s, me).start()

    def z_copy(i, to, frm):
        return pltpu.make_async_remote_copy(
            src_ref=mats.at[cx, frm],
            dst_ref=mats.at[cx, frm],
            send_sem=z_send.at[i],
            recv_sem=z_recv.at[i],
            device_id=at_z(to),
            device_id_type=MESH,
        )

    def x_copy(i, to, frm):
        return pltpu.make_async_remote_copy(
            src_ref=mats.at[frm],
            dst_ref=mats.at[frm],
            send_sem=x_send.at[i],
            recv_sem=x_recv.at[i],
            device_id=at_x(to),
            device_id_type=MESH,
        )

    for i, z in enumerate(z_peers):
        z_copy(i, z, cz).start()
    for i, z in enumerate(z_peers):
        z_copy(i, z, lax.rem(cz + nz - 1 - i, nz)).wait_recv()
    for i, x in enumerate(x_peers):
        x_copy(i, x, cx).start()
    for i, x in enumerate(x_peers):
        x_copy(i, x, lax.rem(cx + nx - 1 - i, nx)).wait_recv()
    keep.wait()

    lane = lax.broadcasted_iota(jnp.int32, (side, 2 * side), 1)
    sign = jnp.where(lane < side, 1.0, -1.0)

    def term(f):
        fields = [waves[s, f, h].astype(jnp.float32) for h in range(2) for s in range(ns)]
        w = jnp.concatenate(fields, axis=0)
        a = mats[f // nz, f % nz].astype(jnp.float32)
        b = jnp.concatenate([a * sign, pltpu.roll(a, side, 1)], axis=0).astype(jnp.bfloat16)
        y = jnp.dot(b, w.astype(jnp.bfloat16), preferred_element_type=jnp.float32)
        numer = jnp.sum(w * y, axis=0, keepdims=True)
        denom = jnp.sum(w * w, axis=0, keepdims=True)
        return numer / denom

    total = jnp.zeros((1, cells), jnp.float32)
    for chunk in range(CHUNKS):
        for i, s in enumerate(sens_peers):
            wave_copy(chunk, i, s, lax.rem(me + ns - 1 - i, ns)).wait_recv()
        total = lax.fori_loop(chunk * step, (chunk + 1) * step, lambda f, t: t + term(f), total)

    def highest_of(value, buf, send, recv, peers, at, mine, count):
        buf[mine] = value

        def copy(i, to, frm):
            return pltpu.make_async_remote_copy(
                src_ref=buf.at[frm],
                dst_ref=buf.at[frm],
                send_sem=send.at[i],
                recv_sem=recv.at[i],
                device_id=at(to),
                device_id_type=MESH,
            )

        for i, p in enumerate(peers):
            copy(i, p, mine).start()
        for i, p in enumerate(peers):
            copy(i, p, lax.rem(mine + count - 1 - i, count)).wait_recv()
        for i, p in enumerate(peers):
            copy(i, p, mine).wait_send()
        return jnp.max(buf[...], axis=0)

    lanes = peak_s.shape[-1]
    peak = functools.reduce(jnp.maximum, [total[:, k : k + lanes] for k in range(0, cells, lanes)])
    peak = highest_of(peak, peak_s, ps_send, ps_recv, sens_peers, at_s, me, ns)
    peak = highest_of(peak, peak_z, pz_send, pz_recv, z_peers, at_z, cz, nz)
    peak = highest_of(peak, peak_x, px_send, px_recv, x_peers, at_x, cx, nx)
    out_ref[...] = total / jnp.max(peak)

    for chunk in range(CHUNKS):
        for i, s in enumerate(sens_peers):
            wave_copy(chunk, i, s, me).wait_send()
    for i, z in enumerate(z_peers):
        z_copy(i, z, cz).wait_send()
    for i, x in enumerate(x_peers):
        x_copy(i, x, cx).wait_send()


def solution(mesh):
    sizes = (4, 16, 4, 2)
    finer = Mesh(mesh.devices.reshape(sizes), ALL)
    nx, nz, ny, nc = sizes
    ns = ny * nc

    def shards(waves, csm):
        freqs, _, rows, wide = waves.shape
        side = csm.shape[-1]
        cells = wide // ns
        dma = pltpu.SemaphoreType.DMA
        out = pl.pallas_call(
            functools.partial(kernel, sizes),
            out_shape=jax.ShapeDtypeStruct((1, cells), jnp.float32),
            in_specs=[pl.BlockSpec(memory_space=pl.ANY)] * 2,
            out_specs=pl.BlockSpec(memory_space=pltpu.VMEM),
            scratch_shapes=[
                pltpu.VMEM((2, side, side), jnp.float32),
                pltpu.VMEM((ns, freqs, 2, rows, cells), jnp.bfloat16),
                pltpu.VMEM((nx, nz, side, 2 * side), jnp.bfloat16),
                pltpu.VMEM((ns, 1, 128), jnp.float32),
                pltpu.VMEM((nz, 1, 128), jnp.float32),
                pltpu.VMEM((nx, 1, 128), jnp.float32),
                dma((2,)),
                dma((CHUNKS, ns - 1)),
                dma((CHUNKS, ns - 1)),
                dma((nz - 1,)),
                dma((nz - 1,)),
                dma((nx - 1,)),
                dma((nx - 1,)),
                dma((ns - 1,)),
                dma((ns - 1,)),
                dma((nz - 1,)),
                dma((nz - 1,)),
                dma((nx - 1,)),
                dma((nx - 1,)),
            ],
            compiler_params=pltpu.CompilerParams(collective_id=0, has_side_effects=True),
        )(waves, csm)
        return out.reshape(cells)

    return jax.shard_map(
        shards,
        mesh=finer,
        in_specs=(P(None, None, SENS, CELL), P(CELL, None, None, None)),
        out_specs=P(ALL),
        check_vma=False,
    )
```

```python
import functools

import jax
import jax.numpy as jnp
from jax import lax
from jax.experimental import pallas as pl
from jax.experimental.pallas import tpu as pltpu
from jax.sharding import Mesh
from jax.sharding import PartitionSpec as P

MESH = pl.DeviceIdType.MESH
CELL = ("cx", "cz")
SENS = ("sy", "sc")
ALL = ("cx", "cz", "sy", "sc")
SIZES = (4, 16, 4, 2)

CHUNKS = (56, 8)
UNROLL = 8
LANES = 128

NX, NZ, NY, NC = SIZES
NS = NY * NC
NEAR = [(0, 0, c, d) for c in range(NY) for d in range(NC)]
ALONG_X = [(a, 0, 0, 0) for a in range(NX)]
ALONG_Z = [(0, b, 0, 0) for b in range(NZ)]
PLANE = [(a, 0, c, d) for a in range(NX) for c in range(NY) for d in range(NC)]
PHASES = (PLANE, ALONG_Z)


def opposite(offset):
    return tuple((n - v) % n for n, v in zip(SIZES, offset))


def far_first(offsets):
    return sorted(offsets[1:], key=lambda o: -sum(min(v, n - v) for n, v in zip(SIZES, o)))


def kernel(
    waves_hbm,
    csm_hbm,
    out_ref,
    csm_vmem,
    waves,
    mats,
    local_sem,
    wave_send,
    wave_recv,
    ring_send,
    ring_recv,
    x_send,
    x_recv,
    *peak_refs,
):
    place = [lax.axis_index(name) for name in ALL]
    cx, cz, sy, sc = place
    me = sy * NC + sc
    freqs = waves.shape[1]
    cells = waves.shape[-1]
    starts = [sum(CHUNKS[:k]) for k in range(len(CHUNKS))]

    def at(offset):
        return {name: p if o == 0 else lax.rem(p + o, n) for name, p, o, n in zip(ALL, place, offset, SIZES)}

    csm_in = pltpu.make_async_copy(csm_hbm.at[0], csm_vmem, local_sem.at[0])
    csm_in.start()

    barrier = pltpu.get_barrier_semaphore()
    greeted = NEAR[1:] + ALONG_X[1:] + [ALONG_Z[1], ALONG_Z[-1]]
    for offset in greeted:
        pl.semaphore_signal(barrier, inc=1, device_id=at(offset), device_id_type=MESH)

    csm_in.wait()
    real, imag = csm_vmem[0], csm_vmem[1]
    side = real.shape[0]
    diag = lax.broadcasted_iota(jnp.int32, (side, side), 0) == lax.broadcasted_iota(jnp.int32, (side, side), 1)
    trace = jnp.sum(jnp.where(diag, real, 0.0))
    mats[cx, cz] = jnp.concatenate([real / trace, imag / trace], axis=1).astype(jnp.bfloat16)

    pl.semaphore_wait(barrier, len(greeted))

    def block(s):
        return pl.ds(pl.multiple_of(s * cells, cells), cells)

    def wave_copy(chunk, offset):
        part = pl.ds(starts[chunk], CHUNKS[chunk])
        i = NEAR.index(offset)
        to = at(offset)
        return pltpu.make_async_remote_copy(
            src_ref=waves_hbm.at[part, :, :, block(to["sy"] * NC + to["sc"])],
            dst_ref=waves.at[me, part],
            send_sem=wave_send.at[chunk, i],
            recv_sem=wave_recv.at[chunk, me],
            device_id=to,
            device_id_type=MESH,
        )

    def wave_arrival(chunk, s):
        part = pl.ds(starts[chunk], CHUNKS[chunk])
        return pltpu.make_async_remote_copy(
            src_ref=waves_hbm.at[part, :, :, block(s)],
            dst_ref=waves.at[s, part],
            send_sem=wave_send.at[chunk, 0],
            recv_sem=wave_recv.at[chunk, s],
            device_id=at(NEAR[1]),
            device_id_type=MESH,
        )

    def own_copy():
        return pltpu.make_async_copy(waves_hbm.at[:, :, :, block(me)], waves.at[me], local_sem.at[1])

    for chunk in range(len(CHUNKS)):
        for offset in far_first(NEAR):
            wave_copy(chunk, offset).start()
    own_copy().start()

    def ring_copy(way, hop):
        here = lax.rem(cz + (NZ - hop + 1 if way == 0 else hop - 1), NZ)
        return pltpu.make_async_remote_copy(
            src_ref=mats.at[cx, here],
            dst_ref=mats.at[cx, here],
            send_sem=ring_send.at[way, hop],
            recv_sem=ring_recv.at[way, hop],
            device_id=at(ALONG_Z[1] if way == 0 else ALONG_Z[-1]),
            device_id_type=MESH,
        )

    def ring_arrival(way, hop):
        here = lax.rem(cz + (NZ - hop if way == 0 else hop), NZ)
        return pltpu.make_async_remote_copy(
            src_ref=mats.at[cx, here],
            dst_ref=mats.at[cx, here],
            send_sem=ring_send.at[way, hop],
            recv_sem=ring_recv.at[way, hop],
            device_id=at(ALONG_Z[1]),
            device_id_type=MESH,
        )

    def x_copy(offset):
        i = ALONG_X.index(offset)
        return pltpu.make_async_remote_copy(
            src_ref=mats.at[cx],
            dst_ref=mats.at[cx],
            send_sem=x_send.at[i],
            recv_sem=x_recv.at[cx],
            device_id=at(offset),
            device_id_type=MESH,
        )

    def x_arrival(offset):
        x = at(offset)["cx"]
        return pltpu.make_async_remote_copy(
            src_ref=mats.at[x],
            dst_ref=mats.at[x],
            send_sem=x_send.at[0],
            recv_sem=x_recv.at[x],
            device_id=at(ALONG_X[1]),
            device_id_type=MESH,
        )

    hops = [(0, h) for h in range(1, NZ // 2 + 1)] + [(1, h) for h in range(1, (NZ + 1) // 2)]
    hops.sort(key=lambda wh: wh[1])
    for way, hop in hops:
        if hop == 1:
            ring_copy(way, hop).start()
    for way, hop in hops:
        ring_arrival(way, hop).wait_recv()
        if (way, hop + 1) in hops:
            ring_copy(way, hop + 1).start()
    for offset in ALONG_X[1:]:
        x_copy(offset).start()
    for offset in ALONG_X[1:]:
        x_arrival(offset).wait_recv()
    own_copy().wait()

    lane = lax.broadcasted_iota(jnp.int32, (side, 2 * side), 1)
    sign = jnp.where(lane < side, 1.0, -1.0)

    def term(f):
        fields = [waves[s, f, h].astype(jnp.float32) for h in range(2) for s in range(NS)]
        w = jnp.concatenate(fields, axis=0).astype(jnp.bfloat16)
        a = mats[f // NZ, f % NZ].astype(jnp.float32)
        b = jnp.concatenate([a * sign, pltpu.roll(a, side, 1)], axis=0).astype(jnp.bfloat16)
        y = jnp.dot(b, w, preferred_element_type=jnp.float32)
        rows = fields[0].shape[0]
        numer = functools.reduce(jnp.add, [v * y[k * rows : (k + 1) * rows] for k, v in enumerate(fields)])
        denom = functools.reduce(jnp.add, [v * v for v in fields])
        return jnp.sum(numer, axis=0, keepdims=True) / jnp.sum(denom, axis=0, keepdims=True)

    total = jnp.zeros((1, cells), jnp.float32)
    for chunk, first in enumerate(starts):
        for offset in far_first(NEAR)[::-1]:
            s = at(offset)
            wave_arrival(chunk, s["sy"] * NC + s["sc"]).wait_recv()
        count = CHUNKS[chunk]
        total = lax.fori_loop(first, first + count, lambda f, t: t + term(f), total, unroll=min(UNROLL, count))

    def peak_copies(phase):
        offsets = PHASES[phase]
        slots, send, recv = peak_refs[3 * phase : 3 * phase + 3]

        def copy(offset):
            i, back = offsets.index(offset), offsets.index(opposite(offset))
            return pltpu.make_async_remote_copy(
                src_ref=slots.at[0],
                dst_ref=slots.at[back],
                send_sem=send.at[i],
                recv_sem=recv.at[back],
                device_id=at(offset),
                device_id_type=MESH,
            )

        return slots, [copy(o) for o in far_first(offsets)]

    peak = functools.reduce(jnp.maximum, [total[:, k : k + LANES] for k in range(0, cells, LANES)])
    for phase in range(len(PHASES)):
        slots, copies = peak_copies(phase)
        slots[0] = peak
        for copy in copies:
            copy.start()
        for offset in far_first(PHASES[phase])[::-1]:
            i = PHASES[phase].index(offset)
            _, send, recv = peak_refs[3 * phase : 3 * phase + 3]
            pltpu.make_async_remote_copy(
                src_ref=slots.at[0],
                dst_ref=slots.at[i],
                send_sem=send.at[i],
                recv_sem=recv.at[i],
                device_id=at(offset),
                device_id_type=MESH,
            ).wait_recv()
        peak = jnp.max(slots[...], axis=0)
    out_ref[...] = total / jnp.max(peak)

    for chunk in range(len(CHUNKS)):
        for offset in NEAR[1:]:
            wave_copy(chunk, offset).wait_send()
    for way, hop in hops:
        ring_copy(way, hop).wait_send()
    for offset in ALONG_X[1:]:
        x_copy(offset).wait_send()
    for phase in range(len(PHASES)):
        for copy in peak_copies(phase)[1]:
            copy.wait_send()


def solution(mesh):
    finer = Mesh(mesh.devices.reshape(SIZES), ALL)

    def shards(waves, csm):
        freqs, _, rows, wide = waves.shape
        side = csm.shape[-1]
        cells = wide // NS
        dma = pltpu.SemaphoreType.DMA
        peaks = [s for p in PHASES for s in (pltpu.VMEM((len(p), 1, LANES), jnp.float32), dma((len(p),)), dma((len(p),)))]
        out = pl.pallas_call(
            kernel,
            out_shape=pltpu.VMEM((1, cells), jnp.float32),
            in_specs=[pl.BlockSpec(memory_space=pl.ANY)] * 2,
            out_specs=pl.BlockSpec(memory_space=pltpu.VMEM),
            scratch_shapes=[
                pltpu.VMEM((2, side, side), jnp.float32),
                pltpu.VMEM((NS, freqs, 2, rows, cells), jnp.bfloat16),
                pltpu.VMEM((NX, NZ, side, 2 * side), jnp.bfloat16),
                dma((2,)),
                dma((len(CHUNKS), NS)),
                dma((len(CHUNKS), NS)),
                dma((2, NZ // 2 + 1)),
                dma((2, NZ // 2 + 1)),
                dma((NX,)),
                dma((NX,)),
                *peaks,
            ],
            compiler_params=pltpu.CompilerParams(collective_id=0, has_side_effects=True),
        )(waves, csm)
        return out.reshape(cells)

    return jax.shard_map(
        shards,
        mesh=finer,
        in_specs=(P(None, None, SENS, CELL), P(CELL, None, None, None)),
        out_specs=P(ALL),
        check_vma=False,
    )
```

```python
import functools

import jax
import jax.numpy as jnp
from jax import lax
from jax.experimental import pallas as pl
from jax.experimental.pallas import tpu as pltpu
from jax.sharding import Mesh
from jax.sharding import PartitionSpec as P

MESH = pl.DeviceIdType.MESH
CELL = ("cx", "cz")
SENS = ("sy", "sc")
ALL = ("cx", "cz", "sy", "sc")
SIZES = (4, 16, 4, 2)

CHUNKS = (8, 48, 8)
STAGED = 1
UNROLL = 8
LANES = 128

NX, NZ, NY, NC = SIZES
NS = NY * NC
NEAR = [(0, 0, c, d) for c in range(NY) for d in range(NC)]
ALONG_X = [(a, 0, 0, 0) for a in range(NX)]
ALONG_Z = [(0, b, 0, 0) for b in range(NZ)]
PLANE = [(a, 0, c, d) for a in range(NX) for c in range(NY) for d in range(NC)]
PHASES = (PLANE, ALONG_Z)


def opposite(offset):
    return tuple((n - v) % n for n, v in zip(SIZES, offset))


def far_first(offsets):
    return sorted(offsets[1:], key=lambda o: -sum(min(v, n - v) for n, v in zip(SIZES, o)))


def kernel(
    waves_hbm,
    csm_hbm,
    out_ref,
    csm_vmem,
    staged,
    waves,
    mats,
    local_sem,
    wave_send,
    wave_recv,
    ring_send,
    ring_recv,
    x_send,
    x_recv,
    *peak_refs,
):
    place = [lax.axis_index(name) for name in ALL]
    cx, cz, sy, sc = place
    me = sy * NC + sc
    freqs = waves.shape[1]
    cells = waves.shape[-1]
    starts = [sum(CHUNKS[:k]) for k in range(len(CHUNKS))]

    def at(offset):
        return {name: p if o == 0 else lax.rem(p + o, n) for name, p, o, n in zip(ALL, place, offset, SIZES)}

    csm_in = pltpu.make_async_copy(csm_hbm.at[0], csm_vmem, local_sem.at[0])
    csm_in.start()

    def stage_copy(chunk):
        part = pl.ds(starts[chunk], CHUNKS[chunk])
        return pltpu.make_async_copy(waves_hbm.at[part], staged.at[part], local_sem.at[2 + chunk])

    for chunk in range(STAGED):
        stage_copy(chunk).start()

    barrier = pltpu.get_barrier_semaphore()
    greeted = NEAR[1:] + ALONG_X[1:] + [ALONG_Z[1], ALONG_Z[-1]]
    for offset in greeted:
        pl.semaphore_signal(barrier, inc=1, device_id=at(offset), device_id_type=MESH)

    csm_in.wait()
    real, imag = csm_vmem[0], csm_vmem[1]
    side = real.shape[0]
    diag = lax.broadcasted_iota(jnp.int32, (side, side), 0) == lax.broadcasted_iota(jnp.int32, (side, side), 1)
    trace = jnp.sum(jnp.where(diag, real, 0.0))
    mats[cx, cz] = jnp.concatenate([real / trace, imag / trace], axis=1).astype(jnp.bfloat16)

    pl.semaphore_wait(barrier, len(greeted))

    def block(s):
        return pl.ds(pl.multiple_of(s * cells, cells), cells)

    def wave_copy(chunk, offset):
        part = pl.ds(starts[chunk], CHUNKS[chunk])
        i = NEAR.index(offset)
        to = at(offset)
        return pltpu.make_async_remote_copy(
            src_ref=(staged if chunk < STAGED else waves_hbm).at[part, :, :, block(to["sy"] * NC + to["sc"])],
            dst_ref=waves.at[me, part],
            send_sem=wave_send.at[chunk, i],
            recv_sem=wave_recv.at[chunk, me],
            device_id=to,
            device_id_type=MESH,
        )

    def wave_arrival(chunk, s):
        part = pl.ds(starts[chunk], CHUNKS[chunk])
        return pltpu.make_async_remote_copy(
            src_ref=(staged if chunk < STAGED else waves_hbm).at[part, :, :, block(s)],
            dst_ref=waves.at[s, part],
            send_sem=wave_send.at[chunk, 0],
            recv_sem=wave_recv.at[chunk, s],
            device_id=at(NEAR[1]),
            device_id_type=MESH,
        )

    def own_copy():
        return pltpu.make_async_copy(waves_hbm.at[:, :, :, block(me)], waves.at[me], local_sem.at[1])

    for chunk in range(len(CHUNKS)):
        if chunk < STAGED:
            stage_copy(chunk).wait()
        for offset in far_first(NEAR):
            wave_copy(chunk, offset).start()
    own_copy().start()

    def ring_copy(way, hop):
        here = lax.rem(cz + (NZ - hop + 1 if way == 0 else hop - 1), NZ)
        return pltpu.make_async_remote_copy(
            src_ref=mats.at[cx, here],
            dst_ref=mats.at[cx, here],
            send_sem=ring_send.at[way, hop],
            recv_sem=ring_recv.at[way, hop],
            device_id=at(ALONG_Z[1] if way == 0 else ALONG_Z[-1]),
            device_id_type=MESH,
        )

    def ring_arrival(way, hop):
        here = lax.rem(cz + (NZ - hop if way == 0 else hop), NZ)
        return pltpu.make_async_remote_copy(
            src_ref=mats.at[cx, here],
            dst_ref=mats.at[cx, here],
            send_sem=ring_send.at[way, hop],
            recv_sem=ring_recv.at[way, hop],
            device_id=at(ALONG_Z[1]),
            device_id_type=MESH,
        )

    def x_copy(offset):
        i = ALONG_X.index(offset)
        return pltpu.make_async_remote_copy(
            src_ref=mats.at[cx],
            dst_ref=mats.at[cx],
            send_sem=x_send.at[i],
            recv_sem=x_recv.at[cx],
            device_id=at(offset),
            device_id_type=MESH,
        )

    def x_arrival(offset):
        x = at(offset)["cx"]
        return pltpu.make_async_remote_copy(
            src_ref=mats.at[x],
            dst_ref=mats.at[x],
            send_sem=x_send.at[0],
            recv_sem=x_recv.at[x],
            device_id=at(ALONG_X[1]),
            device_id_type=MESH,
        )

    hops = [(0, h) for h in range(1, NZ // 2 + 1)] + [(1, h) for h in range(1, (NZ + 1) // 2)]
    hops.sort(key=lambda wh: wh[1])
    for way, hop in hops:
        if hop == 1:
            ring_copy(way, hop).start()
    for way, hop in hops:
        ring_arrival(way, hop).wait_recv()
        if (way, hop + 1) in hops:
            ring_copy(way, hop + 1).start()
    for offset in ALONG_X[1:]:
        x_copy(offset).start()
    for offset in ALONG_X[1:]:
        x_arrival(offset).wait_recv()
    own_copy().wait()

    lane = lax.broadcasted_iota(jnp.int32, (side, 2 * side), 1)
    sign = jnp.where(lane < side, 1.0, -1.0)

    def term(f):
        fields = [waves[s, f, h].astype(jnp.float32) for h in range(2) for s in range(NS)]
        w = jnp.concatenate(fields, axis=0).astype(jnp.bfloat16)
        a = mats[f // NZ, f % NZ].astype(jnp.float32)
        b = jnp.concatenate([a * sign, pltpu.roll(a, side, 1)], axis=0).astype(jnp.bfloat16)
        y = jnp.dot(b, w, preferred_element_type=jnp.float32)
        rows = fields[0].shape[0]
        numer = functools.reduce(jnp.add, [v * y[k * rows : (k + 1) * rows] for k, v in enumerate(fields)])
        denom = functools.reduce(jnp.add, [v * v for v in fields])
        return jnp.sum(numer, axis=0, keepdims=True) / jnp.sum(denom, axis=0, keepdims=True)

    total = jnp.zeros((1, cells), jnp.float32)
    for chunk, first in enumerate(starts):
        for offset in far_first(NEAR)[::-1]:
            s = at(offset)
            wave_arrival(chunk, s["sy"] * NC + s["sc"]).wait_recv()
        count = CHUNKS[chunk]
        total = lax.fori_loop(first, first + count, lambda f, t: t + term(f), total, unroll=min(UNROLL, count))

    def peak_copies(phase):
        offsets = PHASES[phase]
        slots, send, recv = peak_refs[3 * phase : 3 * phase + 3]

        def copy(offset):
            i, back = offsets.index(offset), offsets.index(opposite(offset))
            return pltpu.make_async_remote_copy(
                src_ref=slots.at[0],
                dst_ref=slots.at[back],
                send_sem=send.at[i],
                recv_sem=recv.at[back],
                device_id=at(offset),
                device_id_type=MESH,
            )

        return slots, [copy(o) for o in far_first(offsets)]

    peak = functools.reduce(jnp.maximum, [total[:, k : k + LANES] for k in range(0, cells, LANES)])
    for phase in range(len(PHASES)):
        slots, copies = peak_copies(phase)
        slots[0] = peak
        for copy in copies:
            copy.start()
        for offset in far_first(PHASES[phase])[::-1]:
            i = PHASES[phase].index(offset)
            _, send, recv = peak_refs[3 * phase : 3 * phase + 3]
            pltpu.make_async_remote_copy(
                src_ref=slots.at[0],
                dst_ref=slots.at[i],
                send_sem=send.at[i],
                recv_sem=recv.at[i],
                device_id=at(offset),
                device_id_type=MESH,
            ).wait_recv()
        peak = jnp.max(slots[...], axis=0)
    out_ref[...] = total / jnp.max(peak)

    for chunk in range(len(CHUNKS)):
        for offset in NEAR[1:]:
            wave_copy(chunk, offset).wait_send()
    for way, hop in hops:
        ring_copy(way, hop).wait_send()
    for offset in ALONG_X[1:]:
        x_copy(offset).wait_send()
    for phase in range(len(PHASES)):
        for copy in peak_copies(phase)[1]:
            copy.wait_send()


def solution(mesh):
    finer = Mesh(mesh.devices.reshape(SIZES), ALL)

    def shards(waves, csm):
        freqs, _, rows, wide = waves.shape
        side = csm.shape[-1]
        cells = wide // NS
        dma = pltpu.SemaphoreType.DMA
        peaks = [s for p in PHASES for s in (pltpu.VMEM((len(p), 1, LANES), jnp.float32), dma((len(p),)), dma((len(p),)))]
        out = pl.pallas_call(
            kernel,
            out_shape=pltpu.VMEM((1, cells), jnp.float32),
            in_specs=[pl.BlockSpec(memory_space=pl.ANY)] * 2,
            out_specs=pl.BlockSpec(memory_space=pltpu.VMEM),
            scratch_shapes=[
                pltpu.VMEM((2, side, side), jnp.float32),
                pltpu.VMEM((max(1, sum(CHUNKS[:STAGED])), 2, rows, wide), jnp.bfloat16),
                pltpu.VMEM((NS, freqs, 2, rows, cells), jnp.bfloat16),
                pltpu.VMEM((NX, NZ, side, 2 * side), jnp.bfloat16),
                dma((2 + STAGED,)),
                dma((len(CHUNKS), NS)),
                dma((len(CHUNKS), NS)),
                dma((2, NZ // 2 + 1)),
                dma((2, NZ // 2 + 1)),
                dma((NX,)),
                dma((NX,)),
                *peaks,
            ],
            compiler_params=pltpu.CompilerParams(collective_id=0, has_side_effects=True),
        )(waves, csm)
        return out.reshape(cells)

    return jax.shard_map(
        shards,
        mesh=finer,
        in_specs=(P(None, None, SENS, CELL), P(CELL, None, None, None)),
        out_specs=P(ALL),
        check_vma=False,
    )
```

```python
import functools

import jax
import jax.numpy as jnp
from jax import lax
from jax.experimental import pallas as pl
from jax.experimental.pallas import tpu as pltpu
from jax.sharding import Mesh
from jax.sharding import PartitionSpec as P

MESH = pl.DeviceIdType.MESH
CELL = ("cx", "cz")
SENS = ("sy", "sc")
ALL = ("cx", "cz", "sy", "sc")
SIZES = (4, 16, 4, 2)

CHUNKS = (8, 48, 8)
STAGED = 1
UNROLL = 8
LANES = 128

NX, NZ, NY, NC = SIZES
NS = NY * NC
NEAR = [(0, 0, c, d) for c in range(NY) for d in range(NC)]
ALONG_X = [(a, 0, 0, 0) for a in range(NX)]
ALONG_Z = [(0, b, 0, 0) for b in range(NZ)]
PLANE = [(a, 0, c, d) for a in range(NX) for c in range(NY) for d in range(NC)]
PHASES = (PLANE, ALONG_Z)


def opposite(offset):
    return tuple((n - v) % n for n, v in zip(SIZES, offset))


def far_first(offsets):
    return sorted(offsets[1:], key=lambda o: -sum(min(v, n - v) for n, v in zip(SIZES, o)))


def kernel(
    waves_hbm,
    csm_hbm,
    out_ref,
    csm_vmem,
    staged,
    waves,
    mats,
    local_sem,
    wave_send,
    wave_recv,
    ring_send,
    ring_recv,
    x_send,
    x_recv,
    *peak_refs,
):
    place = [lax.axis_index(name) for name in ALL]
    cx, cz, sy, sc = place
    me = sy * NC + sc
    freqs = waves.shape[1]
    cells = waves.shape[-1]
    starts = [sum(CHUNKS[:k]) for k in range(len(CHUNKS))]

    def at(offset):
        return {name: p if o == 0 else lax.rem(p + o, n) for name, p, o, n in zip(ALL, place, offset, SIZES)}

    csm_in = pltpu.make_async_copy(csm_hbm.at[0], csm_vmem, local_sem.at[0])
    csm_in.start()

    def stage_copy(chunk):
        part = pl.ds(starts[chunk], CHUNKS[chunk])
        return pltpu.make_async_copy(waves_hbm.at[part], staged.at[part], local_sem.at[2 + chunk])

    for chunk in range(STAGED):
        stage_copy(chunk).start()

    barrier = pltpu.get_barrier_semaphore()
    greeted = NEAR[1:] + ALONG_X[1:] + [ALONG_Z[1], ALONG_Z[-1]]
    for offset in greeted:
        pl.semaphore_signal(barrier, inc=1, device_id=at(offset), device_id_type=MESH)

    csm_in.wait()
    real, imag = csm_vmem[0], csm_vmem[1]
    side = real.shape[0]
    diag = lax.broadcasted_iota(jnp.int32, (side, side), 0) == lax.broadcasted_iota(jnp.int32, (side, side), 1)
    trace = jnp.sum(jnp.where(diag, real, 0.0))
    mats[cx, cz] = jnp.concatenate([real / trace, imag / trace], axis=1).astype(jnp.bfloat16)

    pl.semaphore_wait(barrier, len(greeted))

    def block(s):
        return pl.ds(pl.multiple_of(s * cells, cells), cells)

    def wave_copy(chunk, offset):
        part = pl.ds(starts[chunk], CHUNKS[chunk])
        i = NEAR.index(offset)
        to = at(offset)
        return pltpu.make_async_remote_copy(
            src_ref=(staged if chunk < STAGED else waves_hbm).at[part, :, :, block(to["sy"] * NC + to["sc"])],
            dst_ref=waves.at[me, part],
            send_sem=wave_send.at[chunk, i],
            recv_sem=wave_recv.at[chunk, me],
            device_id=to,
            device_id_type=MESH,
        )

    def wave_arrival(chunk, s):
        part = pl.ds(starts[chunk], CHUNKS[chunk])
        return pltpu.make_async_remote_copy(
            src_ref=(staged if chunk < STAGED else waves_hbm).at[part, :, :, block(s)],
            dst_ref=waves.at[s, part],
            send_sem=wave_send.at[chunk, 0],
            recv_sem=wave_recv.at[chunk, s],
            device_id=at(NEAR[1]),
            device_id_type=MESH,
        )

    def own_copy():
        return pltpu.make_async_copy(waves_hbm.at[:, :, :, block(me)], waves.at[me], local_sem.at[1])

    for chunk in range(len(CHUNKS)):
        if chunk < STAGED:
            stage_copy(chunk).wait()
        for offset in far_first(NEAR):
            wave_copy(chunk, offset).start()
    own_copy().start()

    def ring_copy(way, hop):
        here = lax.rem(cz + (NZ - hop + 1 if way == 0 else hop - 1), NZ)
        return pltpu.make_async_remote_copy(
            src_ref=mats.at[cx, here],
            dst_ref=mats.at[cx, here],
            send_sem=ring_send.at[way, hop],
            recv_sem=ring_recv.at[way, hop],
            device_id=at(ALONG_Z[1] if way == 0 else ALONG_Z[-1]),
            device_id_type=MESH,
        )

    def ring_arrival(way, hop):
        here = lax.rem(cz + (NZ - hop if way == 0 else hop), NZ)
        return pltpu.make_async_remote_copy(
            src_ref=mats.at[cx, here],
            dst_ref=mats.at[cx, here],
            send_sem=ring_send.at[way, hop],
            recv_sem=ring_recv.at[way, hop],
            device_id=at(ALONG_Z[1]),
            device_id_type=MESH,
        )

    def x_copy(offset):
        i = ALONG_X.index(offset)
        return pltpu.make_async_remote_copy(
            src_ref=mats.at[cx],
            dst_ref=mats.at[cx],
            send_sem=x_send.at[i],
            recv_sem=x_recv.at[cx],
            device_id=at(offset),
            device_id_type=MESH,
        )

    def x_arrival(offset):
        x = at(offset)["cx"]
        return pltpu.make_async_remote_copy(
            src_ref=mats.at[x],
            dst_ref=mats.at[x],
            send_sem=x_send.at[0],
            recv_sem=x_recv.at[x],
            device_id=at(ALONG_X[1]),
            device_id_type=MESH,
        )

    hops = [(0, h) for h in range(1, NZ // 2 + 1)] + [(1, h) for h in range(1, (NZ + 1) // 2)]
    hops.sort(key=lambda wh: wh[1])
    for way, hop in hops:
        if hop == 1:
            ring_copy(way, hop).start()
    for way, hop in hops:
        ring_arrival(way, hop).wait_recv()
        if (way, hop + 1) in hops:
            ring_copy(way, hop + 1).start()
    for offset in ALONG_X[1:]:
        x_copy(offset).start()
    for offset in ALONG_X[1:]:
        x_arrival(offset).wait_recv()
    own_copy().wait()

    lane = lax.broadcasted_iota(jnp.int32, (side, 2 * side), 1)
    sign = jnp.where(lane < side, 1.0, -1.0)

    def term(f):
        fields = [waves[s, f, h].astype(jnp.float32) for h in range(2) for s in range(NS)]
        w = jnp.concatenate(fields, axis=0).astype(jnp.bfloat16)
        a = mats[f // NZ, f % NZ].astype(jnp.float32)
        b = jnp.concatenate([a * sign, pltpu.roll(a, side, 1)], axis=0).astype(jnp.bfloat16)
        y = jnp.dot(b, w, preferred_element_type=jnp.float32)
        rows = fields[0].shape[0]
        numer = functools.reduce(jnp.add, [v * y[k * rows : (k + 1) * rows] for k, v in enumerate(fields)])
        denom = functools.reduce(jnp.add, [v * v for v in fields])
        return jnp.sum(numer, axis=0, keepdims=True) / jnp.sum(denom, axis=0, keepdims=True)

    total = jnp.zeros((1, cells), jnp.float32)
    for chunk, first in enumerate(starts):
        for offset in far_first(NEAR)[::-1]:
            s = at(offset)
            wave_arrival(chunk, s["sy"] * NC + s["sc"]).wait_recv()
        count = CHUNKS[chunk]
        total = lax.fori_loop(first, first + count, lambda f, t: t + term(f), total, unroll=min(UNROLL, count))

    def peak_copies(phase):
        offsets = PHASES[phase]
        slots, send, recv = peak_refs[3 * phase : 3 * phase + 3]

        def copy(offset):
            i, back = offsets.index(offset), offsets.index(opposite(offset))
            return pltpu.make_async_remote_copy(
                src_ref=slots.at[0],
                dst_ref=slots.at[back],
                send_sem=send.at[i],
                recv_sem=recv,
                device_id=at(offset),
                device_id_type=MESH,
            )

        return slots, [copy(o) for o in far_first(offsets)]

    peak = functools.reduce(jnp.maximum, [total[:, k : k + LANES] for k in range(0, cells, LANES)])
    for phase in range(len(PHASES)):
        slots, copies = peak_copies(phase)
        slots[0] = peak
        for copy in copies:
            copy.start()
        arrived = slots.at[pl.ds(1, len(copies))]
        pltpu.make_async_remote_copy(
            src_ref=arrived,
            dst_ref=arrived,
            send_sem=peak_refs[3 * phase + 1].at[0],
            recv_sem=peak_refs[3 * phase + 2],
            device_id=at(PHASES[phase][1]),
            device_id_type=MESH,
        ).wait_recv()
        peak = jnp.max(slots[...], axis=0)
    out_ref[...] = total / jnp.max(peak)

    for chunk in range(len(CHUNKS)):
        for offset in NEAR[1:]:
            wave_copy(chunk, offset).wait_send()
    for way, hop in hops:
        ring_copy(way, hop).wait_send()
    for offset in ALONG_X[1:]:
        x_copy(offset).wait_send()
    for phase in range(len(PHASES)):
        for copy in peak_copies(phase)[1]:
            copy.wait_send()


def solution(mesh):
    finer = Mesh(mesh.devices.reshape(SIZES), ALL)

    def shards(waves, csm):
        freqs, _, rows, wide = waves.shape
        side = csm.shape[-1]
        cells = wide // NS
        dma = pltpu.SemaphoreType.DMA
        peaks = [s for p in PHASES for s in (pltpu.VMEM((len(p), 1, LANES), jnp.float32), dma((len(p),)), dma)]
        out = pl.pallas_call(
            kernel,
            out_shape=pltpu.VMEM((1, cells), jnp.float32),
            in_specs=[pl.BlockSpec(memory_space=pl.ANY)] * 2,
            out_specs=pl.BlockSpec(memory_space=pltpu.VMEM),
            scratch_shapes=[
                pltpu.VMEM((2, side, side), jnp.float32),
                pltpu.VMEM((max(1, sum(CHUNKS[:STAGED])), 2, rows, wide), jnp.bfloat16),
                pltpu.VMEM((NS, freqs, 2, rows, cells), jnp.bfloat16),
                pltpu.VMEM((NX, NZ, side, 2 * side), jnp.bfloat16),
                dma((2 + STAGED,)),
                dma((len(CHUNKS), NS)),
                dma((len(CHUNKS), NS)),
                dma((2, NZ // 2 + 1)),
                dma((2, NZ // 2 + 1)),
                dma((NX,)),
                dma((NX,)),
                *peaks,
            ],
            compiler_params=pltpu.CompilerParams(collective_id=0, has_side_effects=True),
        )(waves, csm)
        return out.reshape(cells)

    return jax.shard_map(
        shards,
        mesh=finer,
        in_specs=(P(None, None, SENS, CELL), P(CELL, None, None, None)),
        out_specs=P(ALL),
        check_vma=False,
    )
```

```python
import functools

import jax
import jax.numpy as jnp
from jax import lax
from jax.experimental import pallas as pl
from jax.experimental.pallas import tpu as pltpu
from jax.sharding import Mesh
from jax.sharding import PartitionSpec as P

MESH = pl.DeviceIdType.MESH
CELL = ("cx", "cz")
SENS = ("sy", "sc")
ALL = ("cx", "cz", "sy", "sc")
SIZES = (4, 16, 4, 2)

CHUNKS = (8, 48, 8)
STAGED = 1
UNROLL = 8
LANES = 128

NX, NZ, NY, NC = SIZES
NS = NY * NC
NEAR = [(0, 0, c, d) for c in range(NY) for d in range(NC)]
ALONG_X = [(a, 0, 0, 0) for a in range(NX)]
ALONG_Z = [(0, b, 0, 0) for b in range(NZ)]
PLANE = [(a, 0, c, d) for a in range(NX) for c in range(NY) for d in range(NC)]
PHASES = (PLANE, ALONG_Z)


def opposite(offset):
    return tuple((n - v) % n for n, v in zip(SIZES, offset))


def far_first(offsets):
    return sorted(offsets[1:], key=lambda o: -sum(min(v, n - v) for n, v in zip(SIZES, o)))


def kernel(
    waves_hbm,
    csm_hbm,
    out_ref,
    csm_vmem,
    staged,
    waves,
    mats,
    local_sem,
    wave_send,
    wave_recv,
    ring_send,
    ring_recv,
    x_send,
    x_recv,
    *peak_refs,
):
    place = [lax.axis_index(name) for name in ALL]
    cx, cz, sy, sc = place
    me = sy * NC + sc
    freqs = waves.shape[1]
    cells = waves.shape[-1]
    starts = [sum(CHUNKS[:k]) for k in range(len(CHUNKS))]

    def at(offset):
        return {name: p if o == 0 else lax.rem(p + o, n) for name, p, o, n in zip(ALL, place, offset, SIZES)}

    csm_in = pltpu.make_async_copy(csm_hbm.at[0], csm_vmem, local_sem.at[0])
    csm_in.start()

    def stage_copy(chunk):
        part = pl.ds(starts[chunk], CHUNKS[chunk])
        return pltpu.make_async_copy(waves_hbm.at[part], staged.at[part], local_sem.at[2 + chunk])

    for chunk in range(STAGED):
        stage_copy(chunk).start()

    barrier = pltpu.get_barrier_semaphore()
    greeted = NEAR[1:] + ALONG_X[1:] + [ALONG_Z[1], ALONG_Z[-1]]
    for offset in greeted:
        pl.semaphore_signal(barrier, inc=1, device_id=at(offset), device_id_type=MESH)

    csm_in.wait()
    real, imag = csm_vmem[0], csm_vmem[1]
    side = real.shape[0]
    diag = lax.broadcasted_iota(jnp.int32, (side, side), 0) == lax.broadcasted_iota(jnp.int32, (side, side), 1)
    trace = jnp.sum(jnp.where(diag, real, 0.0))
    mats[cx, cz] = jnp.concatenate([real / trace, imag / trace], axis=1).astype(jnp.bfloat16)

    pl.semaphore_wait(barrier, len(greeted))

    def block(s):
        return pl.ds(pl.multiple_of(s * cells, cells), cells)

    def wave_copy(chunk, offset):
        part = pl.ds(starts[chunk], CHUNKS[chunk])
        i = NEAR.index(offset)
        to = at(offset)
        return pltpu.make_async_remote_copy(
            src_ref=(staged if chunk < STAGED else waves_hbm).at[part, :, :, block(to["sy"] * NC + to["sc"])],
            dst_ref=waves.at[me, part],
            send_sem=wave_send.at[chunk, i],
            recv_sem=wave_recv.at[chunk, me],
            device_id=to,
            device_id_type=MESH,
        )

    def wave_arrival(chunk, s):
        part = pl.ds(starts[chunk], CHUNKS[chunk])
        return pltpu.make_async_remote_copy(
            src_ref=(staged if chunk < STAGED else waves_hbm).at[part, :, :, block(s)],
            dst_ref=waves.at[s, part],
            send_sem=wave_send.at[chunk, 0],
            recv_sem=wave_recv.at[chunk, s],
            device_id=at(NEAR[1]),
            device_id_type=MESH,
        )

    def own_copy():
        return pltpu.make_async_copy(waves_hbm.at[:, :, :, block(me)], waves.at[me], local_sem.at[1])

    for chunk in range(len(CHUNKS)):
        if chunk < STAGED:
            stage_copy(chunk).wait()
        for offset in far_first(NEAR):
            wave_copy(chunk, offset).start()
    own_copy().start()

    def ring_copy(way, hop):
        here = lax.rem(cz + (NZ - hop + 1 if way == 0 else hop - 1), NZ)
        return pltpu.make_async_remote_copy(
            src_ref=mats.at[cx, here],
            dst_ref=mats.at[cx, here],
            send_sem=ring_send.at[way, hop],
            recv_sem=ring_recv.at[way, hop],
            device_id=at(ALONG_Z[1] if way == 0 else ALONG_Z[-1]),
            device_id_type=MESH,
        )

    def ring_arrival(way, hop):
        here = lax.rem(cz + (NZ - hop if way == 0 else hop), NZ)
        return pltpu.make_async_remote_copy(
            src_ref=mats.at[cx, here],
            dst_ref=mats.at[cx, here],
            send_sem=ring_send.at[way, hop],
            recv_sem=ring_recv.at[way, hop],
            device_id=at(ALONG_Z[1]),
            device_id_type=MESH,
        )

    def x_copy(offset):
        i = ALONG_X.index(offset)
        return pltpu.make_async_remote_copy(
            src_ref=mats.at[cx],
            dst_ref=mats.at[cx],
            send_sem=x_send.at[i],
            recv_sem=x_recv.at[cx],
            device_id=at(offset),
            device_id_type=MESH,
        )

    def x_arrival(offset):
        x = at(offset)["cx"]
        return pltpu.make_async_remote_copy(
            src_ref=mats.at[x],
            dst_ref=mats.at[x],
            send_sem=x_send.at[0],
            recv_sem=x_recv.at[x],
            device_id=at(ALONG_X[1]),
            device_id_type=MESH,
        )

    hops = [(0, h) for h in range(1, NZ // 2 + 1)] + [(1, h) for h in range(1, (NZ + 1) // 2)]
    hops.sort(key=lambda wh: wh[1])
    for way, hop in hops:
        if hop == 1:
            ring_copy(way, hop).start()
    for way, hop in hops:
        ring_arrival(way, hop).wait_recv()
        if (way, hop + 1) in hops:
            ring_copy(way, hop + 1).start()
    for offset in ALONG_X[1:]:
        x_copy(offset).start()
    for offset in ALONG_X[1:]:
        x_arrival(offset).wait_recv()
    own_copy().wait()

    lane = lax.broadcasted_iota(jnp.int32, (side, 2 * side), 1)
    sign = jnp.where(lane < side, 1.0, -1.0)

    def term(f):
        fields = [waves[s, f, h].astype(jnp.float32) for h in range(2) for s in range(NS)]
        w = jnp.concatenate(fields, axis=0).astype(jnp.bfloat16)
        a = mats[f // NZ, f % NZ].astype(jnp.float32)
        b = jnp.concatenate([a * sign, pltpu.roll(a, side, 1)], axis=0).astype(jnp.bfloat16)
        y = jnp.dot(b, w, preferred_element_type=jnp.float32)
        rows = fields[0].shape[0]
        numer = functools.reduce(jnp.add, [v * y[k * rows : (k + 1) * rows] for k, v in enumerate(fields)])
        denom = functools.reduce(jnp.add, [v * v for v in fields])
        return jnp.sum(numer, axis=0, keepdims=True) / jnp.sum(denom, axis=0, keepdims=True)

    total = jnp.zeros((1, cells), jnp.float32)
    for chunk, first in enumerate(starts):
        for offset in far_first(NEAR)[::-1]:
            s = at(offset)
            wave_arrival(chunk, s["sy"] * NC + s["sc"]).wait_recv()
        count = CHUNKS[chunk]
        total = lax.fori_loop(first, first + count, lambda f, t: t + term(f), total, unroll=min(UNROLL, count))

    def peak_copies(phase):
        offsets = PHASES[phase]
        slots, send, recv = peak_refs[3 * phase : 3 * phase + 3]

        def copy(offset):
            back = offsets.index(opposite(offset))
            return pltpu.make_async_remote_copy(
                src_ref=slots.at[0],
                dst_ref=slots.at[back],
                send_sem=send,
                recv_sem=recv,
                device_id=at(offset),
                device_id_type=MESH,
            )

        return slots, [copy(o) for o in far_first(offsets)]

    def sent_before():
        for chunk in range(len(CHUNKS)):
            for offset in NEAR[1:]:
                wave_copy(chunk, offset).wait_send()
        for way, hop in hops:
            ring_copy(way, hop).wait_send()
        for offset in ALONG_X[1:]:
            x_copy(offset).wait_send()

    peak = functools.reduce(jnp.maximum, [total[:, k : k + LANES] for k in range(0, cells, LANES)])
    for phase in range(len(PHASES)):
        slots, copies = peak_copies(phase)
        slots[0] = peak
        for copy in copies:
            copy.start()
        if phase == 0:
            sent_before()
        arrived = slots.at[pl.ds(1, len(copies))]
        everyone = pltpu.make_async_remote_copy(
            src_ref=arrived,
            dst_ref=arrived,
            send_sem=peak_refs[3 * phase + 1],
            recv_sem=peak_refs[3 * phase + 2],
            device_id=at(PHASES[phase][1]),
            device_id_type=MESH,
        )
        everyone.wait_send()
        everyone.wait_recv()
        peak = jnp.max(slots[...], axis=0)
    out_ref[...] = total / jnp.max(peak)


def solution(mesh):
    finer = Mesh(mesh.devices.reshape(SIZES), ALL)

    def shards(waves, csm):
        freqs, _, rows, wide = waves.shape
        side = csm.shape[-1]
        cells = wide // NS
        dma = pltpu.SemaphoreType.DMA
        peaks = [s for p in PHASES for s in (pltpu.VMEM((len(p), 1, LANES), jnp.float32), dma, dma)]
        out = pl.pallas_call(
            kernel,
            out_shape=pltpu.VMEM((1, cells), jnp.float32),
            in_specs=[pl.BlockSpec(memory_space=pl.ANY)] * 2,
            out_specs=pl.BlockSpec(memory_space=pltpu.VMEM),
            scratch_shapes=[
                pltpu.VMEM((2, side, side), jnp.float32),
                pltpu.VMEM((max(1, sum(CHUNKS[:STAGED])), 2, rows, wide), jnp.bfloat16),
                pltpu.VMEM((NS, freqs, 2, rows, cells), jnp.bfloat16),
                pltpu.VMEM((NX, NZ, side, 2 * side), jnp.bfloat16),
                dma((2 + STAGED,)),
                dma((len(CHUNKS), NS)),
                dma((len(CHUNKS), NS)),
                dma((2, NZ // 2 + 1)),
                dma((2, NZ // 2 + 1)),
                dma((NX,)),
                dma((NX,)),
                *peaks,
            ],
            compiler_params=pltpu.CompilerParams(collective_id=0, has_side_effects=True),
        )(waves, csm)
        return out.reshape(cells)

    return jax.shard_map(
        shards,
        mesh=finer,
        in_specs=(P(None, None, SENS, CELL), P(CELL, None, None, None)),
        out_specs=P(ALL),
        check_vma=False,
    )
```

```python
import functools

import jax
import jax.numpy as jnp
from jax import lax
from jax.experimental import pallas as pl
from jax.experimental.pallas import tpu as pltpu
from jax.sharding import Mesh
from jax.sharding import PartitionSpec as P

MESH = pl.DeviceIdType.MESH
CELL = ("cx", "cz")
SENS = ("sy", "sc")
ALL = ("cx", "cz", "sy", "sc")
SIZES = (4, 16, 4, 2)

CHUNKS = (56, 8)
UNROLL = 8
LANES = 128

NX, NZ, NY, NC = SIZES
NS = NY * NC
NEAR = [(0, 0, c, d) for c in range(NY) for d in range(NC)]
ALONG_X = [(a, 0, 0, 0) for a in range(NX)]
ALONG_Z = [(0, b, 0, 0) for b in range(NZ)]
PLANE = [(a, 0, c, d) for a in range(NX) for c in range(NY) for d in range(NC)]
PHASES = (PLANE, ALONG_Z)


def opposite(offset):
    return tuple((n - v) % n for n, v in zip(SIZES, offset))


def far_first(offsets):
    return sorted(offsets[1:], key=lambda o: -sum(min(v, n - v) for n, v in zip(SIZES, o)))


def kernel(
    waves_hbm,
    csm_hbm,
    out_ref,
    csm_vmem,
    waves,
    mats,
    local_sem,
    wave_send,
    wave_recv,
    ring_send,
    ring_recv,
    x_send,
    x_recv,
    *peak_refs,
):
    place = [lax.axis_index(name) for name in ALL]
    cx, cz, sy, sc = place
    me = sy * NC + sc
    freqs = waves.shape[1]
    cells = waves.shape[-1]
    starts = [sum(CHUNKS[:k]) for k in range(len(CHUNKS))]

    def at(offset):
        return {name: p if o == 0 else lax.rem(p + o, n) for name, p, o, n in zip(ALL, place, offset, SIZES)}

    csm_in = pltpu.make_async_copy(csm_hbm.at[0], csm_vmem, local_sem.at[0])
    csm_in.start()

    barrier = pltpu.get_barrier_semaphore()
    greeted = NEAR[1:] + ALONG_X[1:] + [ALONG_Z[1], ALONG_Z[-1]]
    for offset in greeted:
        pl.semaphore_signal(barrier, inc=1, device_id=at(offset), device_id_type=MESH)

    csm_in.wait()
    real, imag = csm_vmem[0], csm_vmem[1]
    side = real.shape[0]
    diag = lax.broadcasted_iota(jnp.int32, (side, side), 0) == lax.broadcasted_iota(jnp.int32, (side, side), 1)
    trace = jnp.sum(jnp.where(diag, real, 0.0))
    mats[cx, cz] = jnp.concatenate([real / trace, imag / trace], axis=1).astype(jnp.bfloat16)

    pl.semaphore_wait(barrier, len(greeted))

    def block(s):
        return pl.ds(pl.multiple_of(s * cells, cells), cells)

    def wave_copy(chunk, offset):
        part = pl.ds(starts[chunk], CHUNKS[chunk])
        i = NEAR.index(offset)
        to = at(offset)
        return pltpu.make_async_remote_copy(
            src_ref=waves_hbm.at[part, :, :, block(to["sy"] * NC + to["sc"])],
            dst_ref=waves.at[me, part],
            send_sem=wave_send.at[chunk, i],
            recv_sem=wave_recv.at[chunk],
            device_id=to,
            device_id_type=MESH,
        )

    def wave_arrival(chunk):
        part = pl.ds(starts[chunk], CHUNKS[chunk])
        return pltpu.make_async_remote_copy(
            src_ref=waves.at[pl.ds(0, NS - 1), part],
            dst_ref=waves.at[pl.ds(0, NS - 1), part],
            send_sem=wave_send.at[chunk, 0],
            recv_sem=wave_recv.at[chunk],
            device_id=at(NEAR[1]),
            device_id_type=MESH,
        )

    def own_copy():
        return pltpu.make_async_copy(waves_hbm.at[:, :, :, block(me)], waves.at[me], local_sem.at[1])

    for chunk in range(len(CHUNKS)):
        for offset in far_first(NEAR):
            wave_copy(chunk, offset).start()
    own_copy().start()

    def ring_copy(way, hop):
        here = lax.rem(cz + (NZ - hop + 1 if way == 0 else hop - 1), NZ)
        return pltpu.make_async_remote_copy(
            src_ref=mats.at[cx, here],
            dst_ref=mats.at[cx, here],
            send_sem=ring_send.at[way, hop],
            recv_sem=ring_recv.at[way, hop],
            device_id=at(ALONG_Z[1] if way == 0 else ALONG_Z[-1]),
            device_id_type=MESH,
        )

    def ring_arrival(way, hop):
        here = lax.rem(cz + (NZ - hop if way == 0 else hop), NZ)
        return pltpu.make_async_remote_copy(
            src_ref=mats.at[cx, here],
            dst_ref=mats.at[cx, here],
            send_sem=ring_send.at[way, hop],
            recv_sem=ring_recv.at[way, hop],
            device_id=at(ALONG_Z[1]),
            device_id_type=MESH,
        )

    def x_copy(offset):
        i = ALONG_X.index(offset)
        return pltpu.make_async_remote_copy(
            src_ref=mats.at[cx],
            dst_ref=mats.at[cx],
            send_sem=x_send.at[i],
            recv_sem=x_recv.at[cx],
            device_id=at(offset),
            device_id_type=MESH,
        )

    def x_arrival(offset):
        x = at(offset)["cx"]
        return pltpu.make_async_remote_copy(
            src_ref=mats.at[x],
            dst_ref=mats.at[x],
            send_sem=x_send.at[0],
            recv_sem=x_recv.at[x],
            device_id=at(ALONG_X[1]),
            device_id_type=MESH,
        )

    hops = [(0, h) for h in range(1, NZ // 2 + 1)] + [(1, h) for h in range(1, (NZ + 1) // 2)]
    hops.sort(key=lambda wh: wh[1])
    for way, hop in hops:
        if hop == 1:
            ring_copy(way, hop).start()
    for way, hop in hops:
        ring_arrival(way, hop).wait_recv()
        if (way, hop + 1) in hops:
            ring_copy(way, hop + 1).start()
    for offset in ALONG_X[1:]:
        x_copy(offset).start()
    for offset in ALONG_X[1:]:
        x_arrival(offset).wait_recv()
    own_copy().wait()

    lane = lax.broadcasted_iota(jnp.int32, (side, 2 * side), 1)
    sign = jnp.where(lane < side, 1.0, -1.0)

    def term(f):
        fields = [waves[s, f, h].astype(jnp.float32) for h in range(2) for s in range(NS)]
        w = jnp.concatenate(fields, axis=0).astype(jnp.bfloat16)
        a = mats[f // NZ, f % NZ].astype(jnp.float32)
        b = jnp.concatenate([a * sign, pltpu.roll(a, side, 1)], axis=0).astype(jnp.bfloat16)
        y = jnp.dot(b, w, preferred_element_type=jnp.float32)
        rows = fields[0].shape[0]
        numer = functools.reduce(jnp.add, [v * y[k * rows : (k + 1) * rows] for k, v in enumerate(fields)])
        denom = functools.reduce(jnp.add, [v * v for v in fields])
        return jnp.sum(numer, axis=0, keepdims=True) / jnp.sum(denom, axis=0, keepdims=True)

    total = jnp.zeros((1, cells), jnp.float32)
    for chunk, first in enumerate(starts):
        wave_arrival(chunk).wait_recv()
        count = CHUNKS[chunk]
        total = lax.fori_loop(first, first + count, lambda f, t: t + term(f), total, unroll=min(UNROLL, count))

    def peak_copies(phase):
        offsets = PHASES[phase]
        slots, send, recv = peak_refs[3 * phase : 3 * phase + 3]

        def copy(offset):
            back = offsets.index(opposite(offset))
            return pltpu.make_async_remote_copy(
                src_ref=slots.at[0],
                dst_ref=slots.at[back],
                send_sem=send,
                recv_sem=recv,
                device_id=at(offset),
                device_id_type=MESH,
            )

        return slots, [copy(o) for o in far_first(offsets)]

    def sent_before():
        for chunk in range(len(CHUNKS)):
            for offset in NEAR[1:]:
                wave_copy(chunk, offset).wait_send()
        for way, hop in hops:
            ring_copy(way, hop).wait_send()
        for offset in ALONG_X[1:]:
            x_copy(offset).wait_send()

    peak = functools.reduce(jnp.maximum, [total[:, k : k + LANES] for k in range(0, cells, LANES)])
    for phase in range(len(PHASES)):
        slots, copies = peak_copies(phase)
        slots[0] = peak
        for copy in copies:
            copy.start()
        if phase == 0:
            sent_before()
        arrived = slots.at[pl.ds(1, len(copies))]
        everyone = pltpu.make_async_remote_copy(
            src_ref=arrived,
            dst_ref=arrived,
            send_sem=peak_refs[3 * phase + 1],
            recv_sem=peak_refs[3 * phase + 2],
            device_id=at(PHASES[phase][1]),
            device_id_type=MESH,
        )
        everyone.wait_send()
        everyone.wait_recv()
        peak = jnp.max(slots[...], axis=0)
    out_ref[...] = total / jnp.max(peak)


def solution(mesh):
    finer = Mesh(mesh.devices.reshape(SIZES), ALL)

    def shards(waves, csm):
        freqs, _, rows, wide = waves.shape
        side = csm.shape[-1]
        cells = wide // NS
        dma = pltpu.SemaphoreType.DMA
        peaks = [s for p in PHASES for s in (pltpu.VMEM((len(p), 1, LANES), jnp.float32), dma, dma)]
        out = pl.pallas_call(
            kernel,
            out_shape=pltpu.VMEM((1, cells), jnp.float32),
            in_specs=[pl.BlockSpec(memory_space=pl.ANY)] * 2,
            out_specs=pl.BlockSpec(memory_space=pltpu.VMEM),
            scratch_shapes=[
                pltpu.VMEM((2, side, side), jnp.float32),
                pltpu.VMEM((NS, freqs, 2, rows, cells), jnp.bfloat16),
                pltpu.VMEM((NX, NZ, side, 2 * side), jnp.bfloat16),
                dma((2,)),
                dma((len(CHUNKS), NS)),
                dma((len(CHUNKS),)),
                dma((2, NZ // 2 + 1)),
                dma((2, NZ // 2 + 1)),
                dma((NX,)),
                dma((NX,)),
                *peaks,
            ],
            compiler_params=pltpu.CompilerParams(collective_id=0, has_side_effects=True),
        )(waves, csm)
        return out.reshape(cells)

    return jax.shard_map(
        shards,
        mesh=finer,
        in_specs=(P(None, None, SENS, CELL), P(CELL, None, None, None)),
        out_specs=P(ALL),
        check_vma=False,
    )
```
